32 devices in a mesh: dp: 16 (over z, x, core), tp: 2 (over y).
Axes of the slice: x: 2, y: 2, z: 4, core: 2. Of those that a mesh axis runs over, the one named last changes fastest.
Arguments:
- gate_pre: bfloat16 [12288, 7168], P('dp', 'tp'), may hold values from -6 to 6
- up_pre: bfloat16 [12288, 7168], P('dp', 'tp'), may hold values from -6 to 6
- target: bfloat16 [12288, 2048], P('dp', 'tp'), may hold values from -6 to 6
- norm_gain: float32 [2048], P('tp'), may hold values from 0.5 to 1.5
- weight: bfloat16 [16, 7168, 2048], P('dp', 'tp'), may hold values from -6 to 6
- round_index: int32 [1], replicated, may hold values from 0 to 9999
Outputs:
- normed: bfloat16 [12288, 2048], P('dp', 'tp')
- mixed: bfloat16 [16, 7168, 2048], P('dp', 'tp')
The draws below stay inside these ranges and needn't reach their ends.
All inputs are finite; a program needn't handle non-finite values.
Results may differ from the reference program's by a relative error of at most 0.001.
The reference program's roundings to bfloat16 on the way (of `hidden`, `grad_out` and `updated`) count: a program that leaves them out, or rounds other values in their place, can miss the bound.
Values may be sent and summed in bfloat16 or wider, within the bound.
A program may use at most 128 MiB of HBM per device.

```python
import math
import jax
import jax.numpy as jnp
from jax import lax

D = 2048
FF = 7168
TOK = 768
TOKENS = 12288
N_DP = 16


def block_scale(key, dims, pieces, smallest, high):
    factor_of, own = 1.0, jax.random.fold_in(key, 6)
    for dim, shards_of in pieces:
        steps = jnp.exp(jax.random.uniform(jax.random.fold_in(own, dim), (shards_of,), jnp.float32, smallest / len(pieces), high / len(pieces)))
        factor_of = factor_of * jnp.repeat(steps, dims[dim] // shards_of).reshape([-1 if axis == dim else 1 for axis in range(len(dims))])
    return factor_of


def centred(key, extent, scale, reach, split=(), kind=jnp.bfloat16):
    drawn = jax.random.normal(key, extent, jnp.float32) * scale
    if len(split) > 0:
        drawn = block_scale(key, extent, split, -0.22, 0.18) * drawn
    return jnp.clip(drawn, min=-reach, max=reach).astype(kind)


def setup_inputs(seed: int = 0) -> dict:
    arg_keys = jax.random.split(jax.random.key(seed), 7)
    gate_pre = centred(arg_keys[0], (TOKENS, FF), 1.0, 6.0, ((0, 16), (1, 2)))
    up_pre = centred(arg_keys[1], (TOKENS, FF), 1.0, 6.0, ((0, 16), (1, 2)))
    target = centred(arg_keys[2], (TOKENS, D), 1.0, 6.0, ((0, 16), (1, 2)))
    norm_gain = jnp.clip(1.0 + 0.1 * jax.random.normal(arg_keys[3], (D,), jnp.float32), 0.5, 1.5)
    weight = centred(arg_keys[4], (N_DP, FF, D), 1.0, 6.0, ((0, 16), (1, 2)))
    round_index = jax.random.randint(arg_keys[5], (1,), 0, 10000).astype(jnp.int32)
    return {"gate_pre": gate_pre, "up_pre": up_pre, "target": target, "norm_gain": norm_gain, "weight": weight, "round_index": round_index}


EPSILON = 1e-06

def step_rate(round_index):
    phase = (round_index[0] % 1000).astype(jnp.float32) * jnp.float32(2.0 * math.pi / 1000.0)
    return jnp.float32(0.25) * (jnp.float32(0.55) + jnp.float32(0.45) * jnp.cos(phase))

def replica_step(inputs, norm_gain, rate):
    gate_rows, up_rows, target_rows, weight_rows = inputs
    out_scale = FF ** (-0.5)
    hidden = (jax.nn.silu(gate_rows.astype(jnp.float32)) * up_rows.astype(jnp.float32)).astype(jnp.bfloat16)
    summed = jnp.dot(hidden, weight_rows, preferred_element_type=jnp.float32) * out_scale
    inv_rms = lax.rsqrt(lax.optimization_barrier(jnp.mean(summed * summed, axis=1, keepdims=True)) + EPSILON)
    normal = summed * inv_rms
    output = normal * norm_gain
    grad_norm = (output - target_rows.astype(jnp.float32)) * norm_gain
    inner = lax.optimization_barrier(jnp.mean(grad_norm * normal, axis=1, keepdims=True))
    grad_out = (inv_rms * (grad_norm - normal * inner)).astype(jnp.bfloat16)
    weight_grad = lax.dot_general(hidden, grad_out, (((0,), (0,)), ((), ())), preferred_element_type=jnp.float32) * out_scale
    updated = (weight_rows.astype(jnp.float32) - rate * weight_grad).astype(jnp.bfloat16)
    return (output.astype(jnp.bfloat16), updated)

def reference(gate_pre, up_pre, target, norm_gain, weight, round_index):
    gate_blocks = gate_pre.reshape(N_DP, TOK, FF)
    up_blocks = up_pre.reshape(N_DP, TOK, FF)
    target_blocks = target.reshape(N_DP, TOK, D)
    rate = step_rate(round_index)

    def one_replica(inputs):
        return replica_step(inputs, norm_gain, rate)
    normed, updated = lax.map(one_replica, (gate_blocks, up_blocks, target_blocks, weight))
    levels = N_DP.bit_length() - 1
    offset = jnp.left_shift(jnp.int32(1), (round_index[0] % levels).astype(jnp.int32))
    source = ((jnp.arange(N_DP, dtype=jnp.int32) - offset) % N_DP).astype(jnp.int32)
    peer_rows = updated[source]
    mixed = (0.5 * (updated.astype(jnp.float32) + peer_rows.astype(jnp.float32))).astype(jnp.bfloat16)
    return (normed.reshape(N_DP * TOK, D), mixed)
```

```python
import functools
import math

import jax
import jax.numpy as jnp
from jax import lax
from jax.experimental import pallas as pl
from jax.experimental.pallas import tpu as pltpu
from jax.sharding import PartitionSpec as P

EPSILON = 1e-06
MESH = pl.DeviceIdType.MESH
BF16, F32 = jnp.bfloat16, jnp.float32


def step_rate(round_index):
    phase = (round_index[0] % 1000).astype(jnp.float32) * jnp.float32(2.0 * math.pi / 1000.0)
    return jnp.float32(0.25) * (jnp.float32(0.55) + jnp.float32(0.45) * jnp.cos(phase))


def divisor(size, limits):
    for limit in limits:
        if size % limit == 0:
            return limit
    return size


def kernel(
    offset, early, chunk, tile, block, scale,
    rate_ref, gain_ref, gate_hbm, up_hbm, target_hbm, weight_hbm,
    normed_hbm, mixed_hbm,
    held, inbox, hidden, gate_buf, up_buf, high_out, low_out, high_in, low_in,
    share, goal, grads, coarse, normed, turned, flat, stat_out, stat_in,
    gate_sem, up_sem, weight_sem, goal_sem, high_send, high_recv, low_send, low_recv,
    stat_send, stat_recv, grad_send, grad_recv, block_send, block_recv, mixed_sem, normed_sem,
):
    tp, rows, part = held.shape
    tokens = hidden.shape[0]
    width = tp * part
    pieces, tiles, blocks = tokens // chunk, part // tile, rows // block
    me, mine = lax.axis_index("tp"), lax.axis_index("dp")
    replicas = lax.axis_size("dp")
    ahead = {"dp": lax.rem(mine + offset, replicas)}
    behind = {"dp": lax.rem(mine + replicas - offset, replicas)}
    rate = rate_ref[0]

    def peer(k):
        return {"tp": lax.rem(me + k, tp)}

    def columns(k):
        return pl.ds(pl.multiple_of(lax.rem(me + k, tp) * part, part), part)

    def token_rows(i):
        return pl.ds(pl.multiple_of(i * chunk, chunk), chunk)

    def span(i, size):
        return pl.ds(pl.multiple_of(i * size, size), size)

    barrier = pltpu.get_barrier_semaphore()
    for k in range(1, tp):
        pl.semaphore_signal(barrier, inc=1, device_id=peer(k), device_id_type=MESH)
    pl.semaphore_signal(barrier, inc=1, device_id=ahead, device_id_type=MESH)
    pl.semaphore_signal(barrier, inc=1, device_id=behind, device_id_type=MESH)

    def gate_copy(i):
        slot = lax.rem(i, 2)
        return pltpu.make_async_copy(gate_hbm.at[token_rows(i)], gate_buf.at[slot], gate_sem.at[slot])

    def up_copy(i):
        slot = lax.rem(i, 2)
        return pltpu.make_async_copy(up_hbm.at[token_rows(i)], up_buf.at[slot], up_sem.at[slot])

    def weight_copy(k):
        return pltpu.make_async_copy(weight_hbm.at[:, columns(k)], held.at[k], weight_sem.at[k])

    goal_copy = pltpu.make_async_copy(target_hbm, goal, goal_sem)
    gate_copy(0).start()
    up_copy(0).start()
    for k in range(1, tp):
        weight_copy(k).start()
    if pieces > 1:
        gate_copy(1).start()
        up_copy(1).start()
    weight_copy(0).start()
    goal_copy.start()

    def tp_copy(source, landing, send, recv, k, i):
        return pltpu.make_async_remote_copy(
            src_ref=source.at[k - 1, token_rows(i)],
            dst_ref=landing.at[k - 1, token_rows(i)],
            send_sem=send.at[k - 1, i],
            recv_sem=recv.at[k - 1, i],
            device_id=peer(k),
            device_id_type=MESH,
        )

    def high_copy(k, i):
        return tp_copy(high_out, high_in, high_send, high_recv, k, i)

    def low_copy(k, i):
        return tp_copy(low_out, low_in, low_send, low_recv, k, i)

    pl.semaphore_wait(barrier, tp + 1)

    @pl.loop(0, pieces)
    def _(i):
        slot = lax.rem(i, 2)
        gate_copy(i).wait()
        up_copy(i).wait()

        @pl.loop(0, chunk // 16)
        def _(r):
            gate = gate_buf[slot, span(r, 16), :].astype(F32)
            value = gate / (1.0 + jnp.exp(-gate)) * up_buf[slot, span(r, 16), :].astype(F32)
            hidden[pl.ds(pl.multiple_of(i * chunk + r * 16, 16), 16), :] = value.astype(BF16)

        @pl.when(i + 2 < pieces)
        def _():
            gate_copy(i + 2).start()
            up_copy(i + 2).start()

        for k in range(1, tp):

            @pl.when(i == 0)
            def _(k=k):
                weight_copy(k).wait()

        @pl.loop(1, tp)
        def _(k):
            @pl.loop(0, tiles)
            def _(n):
                product = jnp.dot(
                    hidden[token_rows(i), :], held[k, :, span(n, tile)], preferred_element_type=F32
                ) * scale
                top = product.astype(BF16)
                high_out[k - 1, token_rows(i), span(n, tile)] = top
                low_out[k - 1, token_rows(i), span(n, tile)] = (product - top.astype(F32)).astype(BF16)

        for k in range(1, tp):
            high_copy(k, i).start()

    weight_copy(0).wait()
    goal_copy.wait()

    @pl.loop(0, pieces)
    def _(i):
        @pl.loop(0, tiles)
        def _(n):
            share[token_rows(i), span(n, tile)] = jnp.dot(
                hidden[token_rows(i), :], held[0, :, span(n, tile)], preferred_element_type=F32
            ) * scale

    flat[...] = jnp.zeros_like(flat)
    lane = lax.broadcasted_iota(jnp.int32, (16, 128), 1)

    def stat_copy(turn, k, i):
        return pltpu.make_async_remote_copy(
            src_ref=stat_out.at[turn, i],
            dst_ref=stat_in.at[turn, k - 1, i],
            send_sem=stat_send.at[turn, k - 1, i],
            recv_sem=stat_recv.at[turn, k - 1, i],
            device_id=peer(k),
            device_id_type=MESH,
        )

    def add_and_count(turn, landing, i):
        @pl.loop(0, chunk // 16)
        def _(r):
            here = pl.ds(pl.multiple_of(i * chunk + r * 16, 16), 16)
            total = share[here, :]
            for k in range(1, tp):
                total = total + landing[k - 1, here, :].astype(F32)
            share[here, :] = total
            gain = gain_ref[...]
            squares = total * total
            first = jnp.sum(squares, axis=1, keepdims=True)
            second = jnp.sum(squares * (gain * gain), axis=1, keepdims=True)
            third = jnp.sum(total * (goal[here, :].astype(F32) * gain), axis=1, keepdims=True)
            turned[span(r, 16), :] = jnp.where(
                lane == 0, first, jnp.where(lane == 1, second, jnp.where(lane == 2, third, 0.0))
            )

        stat_out[turn, i] = turned[...].T[0:8, :]
        for k in range(1, tp):
            stat_copy(turn, k, i).start()

    def gradient(turn, result, i):
        totals = stat_out[turn, i]
        for k in range(1, tp):
            stat_copy(turn, k, i).wait()
            totals = totals + stat_in[turn, k - 1, i]
        flat[0:8, :] = totals
        turned[...] = flat[...].T

        @pl.loop(0, chunk // 16)
        def _(r):
            here = pl.ds(pl.multiple_of(i * chunk + r * 16, 16), 16)
            sums = turned[span(r, 16), :] * (1.0 / width)
            inv_rms = lax.rsqrt(sums[:, 0:1] + EPSILON)
            inner = inv_rms * (inv_rms * sums[:, 1:2] - sums[:, 2:3])
            gain = gain_ref[...]
            normal = share[here, :] * inv_rms
            output = normal * gain
            grad_norm = (output - goal[here, :].astype(F32)) * gain
            result[here, :] = (inv_rms * (grad_norm - normal * inner)).astype(BF16)
            if turn:
                normed[here, :] = output.astype(BF16)

    def block_copy(k, b):
        return pltpu.make_async_remote_copy(
            src_ref=held.at[k, span(b, block)],
            dst_ref=inbox.at[k, span(b, block)],
            send_sem=block_send.at[k, b],
            recv_sem=block_recv.at[k, b],
            device_id=ahead,
            device_id_type=MESH,
        )

    def update(k, b, grad):
        @pl.loop(0, tiles)
        def _(n):
            weight_grad = lax.dot_general(
                hidden[:, span(b, block)], grad[:, span(n, tile)], (((0,), (0,)), ((), ())),
                preferred_element_type=F32,
            ) * scale
            old = held[k, span(b, block), span(n, tile)].astype(F32)
            held[k, span(b, block), span(n, tile)] = (old - rate * weight_grad).astype(BF16)

        block_copy(k, b).start()

    @pl.loop(0, pieces)
    def _(i):
        for k in range(1, tp):
            high_copy(k, i).wait()
        add_and_count(0, high_in, i)

    for k in range(1, tp):
        for i in range(pieces):
            low_copy(k, i).start()

    @pl.loop(0, pieces)
    def _(i):
        gradient(0, coarse, i)

    @pl.loop(0, early)
    def _(b):
        update(0, b, coarse)

    @pl.loop(0, pieces)
    def _(i):
        for k in range(1, tp):
            low_copy(k, i).wait()
        add_and_count(1, low_in, i)

    def normed_copy(i):
        return pltpu.make_async_copy(normed.at[token_rows(i)], normed_hbm.at[token_rows(i)], normed_sem.at[i])

    def grad_copy(k):
        return pltpu.make_async_remote_copy(
            src_ref=grads.at[0],
            dst_ref=grads.at[tp - k],
            send_sem=grad_send.at[k - 1],
            recv_sem=grad_recv.at[tp - k - 1],
            device_id=peer(k),
            device_id_type=MESH,
        )

    @pl.loop(0, pieces)
    def _(i):
        gradient(1, grads.at[0], i)
        normed_copy(i).start()

    for k in range(1, tp):
        grad_copy(k).start()

    @pl.loop(early, blocks)
    def _(b):
        update(0, b, grads.at[0])

    for k in range(1, tp):
        grad_copy(k).wait()

    @pl.loop(1, tp)
    def _(k):
        @pl.loop(0, blocks)
        def _(b):
            update(k, b, grads.at[k])

    def mixed_copy(k, b):
        return pltpu.make_async_copy(
            held.at[k, span(b, block)], mixed_hbm.at[span(b, block), columns(k)], mixed_sem.at[k, b]
        )

    @pl.loop(0, tp)
    def _(k):
        @pl.loop(0, blocks)
        def _(b):
            block_copy(k, b).wait()

            @pl.loop(0, block // 16)
            def _(r):
                here = pl.ds(pl.multiple_of(b * block + r * 16, 16), 16)
                both = held[k, here, :].astype(F32) + inbox[k, here, :].astype(F32)
                held[k, here, :] = (0.5 * both).astype(BF16)

            mixed_copy(k, b).start()

    @pl.loop(0, pieces)
    def _(i):
        normed_copy(i).wait()

    @pl.loop(0, tp)
    def _(k):
        @pl.loop(0, blocks)
        def _(b):
            mixed_copy(k, b).wait()


def shards(gate_pre, up_pre, target, norm_gain, weight, round_index):
    rate = step_rate(round_index)
    replicas = lax.axis_size("dp")
    levels = replicas.bit_length() - 1
    level = round_index[0] % levels
    tp = lax.axis_size("tp")
    _, rows, width = weight.shape
    tokens = gate_pre.shape[0]
    part = width // tp
    scale = (rows * tp) ** (-0.5)
    chunk = divisor(tokens, (256, 128))
    tile = divisor(part, (256, 128))
    block = divisor(rows, (256, 128))
    pieces, blocks = tokens // chunk, rows // block
    dma = pltpu.SemaphoreType.DMA

    def call(bit):
        early = min(blocks, (8, 4, 4, 2)[min(bit, 3)])
        any_space = pl.BlockSpec(memory_space=pl.ANY)
        return pl.pallas_call(
            functools.partial(kernel, 1 << bit, early, chunk, tile, block, scale),
            out_shape=(
                jax.ShapeDtypeStruct((tokens, part), BF16),
                jax.ShapeDtypeStruct((rows, width), BF16),
            ),
            in_specs=[
                pl.BlockSpec(memory_space=pltpu.SMEM),
                pl.BlockSpec(memory_space=pltpu.VMEM),
            ]
            + [any_space] * 4,
            out_specs=(any_space, any_space),
            scratch_shapes=[
                pltpu.VMEM((tp, rows, part), BF16),
                pltpu.VMEM((tp, rows, part), BF16),
                pltpu.VMEM((tokens, rows), BF16),
                pltpu.VMEM((2, chunk, rows), BF16),
                pltpu.VMEM((2, chunk, rows), BF16),
            ]
            + [pltpu.VMEM((tp - 1, tokens, part), BF16)] * 4
            + [
                pltpu.VMEM((tokens, part), F32),
                pltpu.VMEM((tokens, part), BF16),
                pltpu.VMEM((tp, tokens, part), BF16),
                pltpu.VMEM((tokens, part), BF16),
                pltpu.VMEM((tokens, part), BF16),
                pltpu.VMEM((chunk, 128), F32),
                pltpu.VMEM((128, chunk), F32),
                pltpu.VMEM((2, pieces, 8, chunk), F32),
                pltpu.VMEM((2, tp - 1, pieces, 8, chunk), F32),
                dma((2,)),
                dma((2,)),
                dma((tp,)),
                dma,
            ]
            + [dma((tp - 1, pieces))] * 4
            + [dma((2, tp - 1, pieces))] * 2
            + [dma((tp - 1,))] * 2
            + [dma((tp, blocks))] * 3
            + [dma((pieces,))],
            compiler_params=pltpu.CompilerParams(
                collective_id=bit, has_side_effects=True, vmem_limit_bytes=66_000_000
            ),
            name=f"step_level{bit}",
        )

    def branch(bit):
        def run(*operands):
            return call(bit)(*operands)

        return run

    normed, mixed = lax.switch(
        level,
        [branch(bit) for bit in range(levels)],
        rate[None],
        norm_gain[None, :],
        gate_pre,
        up_pre,
        target,
        weight[0],
    )
    return (normed, mixed[None])


def solution(mesh):
    return jax.shard_map(
        shards,
        mesh=mesh,
        in_specs=(P("dp", "tp"), P("dp", "tp"), P("dp", "tp"), P("tp"), P("dp", "tp", None), P()),
        out_specs=(P("dp", "tp"), P("dp", "tp", None)),
        check_vma=False,
    )
```

```python
import functools
import math

import jax
import jax.numpy as jnp
from jax import lax
from jax.experimental import pallas as pl
from jax.experimental.pallas import tpu as pltpu
from jax.sharding import PartitionSpec as P

EPSILON = 1e-06
MESH = pl.DeviceIdType.MESH
BF16, F32 = jnp.bfloat16, jnp.float32


def step_rate(round_index):
    phase = (round_index[0] % 1000).astype(jnp.float32) * jnp.float32(2.0 * math.pi / 1000.0)
    return jnp.float32(0.25) * (jnp.float32(0.55) + jnp.float32(0.45) * jnp.cos(phase))


def divisor(size, limits):
    for limit in limits:
        if size % limit == 0:
            return limit
    return size


def kernel(
    offset, early_even, early_odd, chunk, group, tile, block, scale,
    rate_ref, gain_ref, gate_hbm, up_hbm, target_hbm, weight_hbm,
    normed, held,
    inbox, hidden, gate_buf, up_buf, high_out, low_out, high_in, low_in,
    share, goal, grads, coarse, turned, flat, stat_out, stat_in,
    gate_sem, up_sem, weight_sem, goal_sem, high_send, high_recv, low_send, low_recv,
    stat_send, stat_recv, grad_send, grad_recv, block_send, block_recv, turn_sem,
):
    tp, rows, part = held.shape
    tokens = hidden.shape[0]
    width = tp * part
    pieces, tiles, blocks = tokens // chunk, part // tile, rows // block
    window, step = min(5, pieces), 64
    me, mine = lax.axis_index("tp"), lax.axis_index("dp")
    replicas = lax.axis_size("dp")
    ahead = {"dp": lax.rem(mine + offset, replicas)}
    behind = {"dp": lax.rem(mine + replicas - offset, replicas)}
    odd = lax.rem(mine, 2)
    partner = {"dp": mine + 1 - 2 * odd}
    early = early_odd * odd + early_even * (1 - odd)
    rate = rate_ref[0]

    def peer(k):
        return {"tp": lax.rem(me + k, tp)}

    def columns(k):
        return pl.ds(pl.multiple_of(lax.rem(me + k, tp) * part, part), part)

    def token_rows(i):
        return pl.ds(pl.multiple_of(i * chunk, chunk), chunk)

    def span(i, size):
        return pl.ds(pl.multiple_of(i * size, size), size)

    barrier = pltpu.get_barrier_semaphore()
    for k in range(1, tp):
        pl.semaphore_signal(barrier, inc=1, device_id=peer(k), device_id_type=MESH)
    pl.semaphore_signal(barrier, inc=1, device_id=ahead, device_id_type=MESH)
    pl.semaphore_signal(barrier, inc=1, device_id=behind, device_id_type=MESH)
    pl.semaphore_signal(barrier, inc=1, device_id=partner, device_id_type=MESH)

    def gate_copy(i):
        slot = lax.rem(i, 2)
        return pltpu.make_async_copy(gate_hbm.at[token_rows(i)], gate_buf.at[slot], gate_sem.at[slot])

    def up_copy(i):
        slot = lax.rem(i, 2)
        return pltpu.make_async_copy(up_hbm.at[token_rows(i)], up_buf.at[slot], up_sem.at[slot])

    def weight_copy(k, n):
        first = lax.rem(me + k, tp) * part + n * tile
        return pltpu.make_async_copy(
            weight_hbm.at[:, pl.ds(pl.multiple_of(first, tile), tile)],
            held.at[k, :, span(n, tile)],
            weight_sem.at[k, n],
        )

    def weight_start(k):
        for n in range(tiles):
            weight_copy(k, n).start()

    goal_copy = pltpu.make_async_copy(target_hbm, goal, goal_sem)
    gate_copy(0).start()
    up_copy(0).start()
    for k in range(1, tp):
        weight_start(k)

    def tp_copy(source, landing, send, recv, k, i):
        return pltpu.make_async_remote_copy(
            src_ref=source.at[k - 1, token_rows(i)],
            dst_ref=landing.at[k - 1, token_rows(i)],
            send_sem=send.at[k - 1, i],
            recv_sem=recv.at[k - 1, i],
            device_id=peer(k),
            device_id_type=MESH,
        )

    def high_copy(k, i):
        return tp_copy(high_out, high_in, high_send, high_recv, k, i)

    def low_copy(k, i):
        return tp_copy(low_out, low_in, low_send, low_recv, k, i)

    def begin(i, more):
        slot = lax.rem(i, 2)
        gate_copy(i).wait()
        up_copy(i).wait()

        @pl.loop(0, chunk // 16)
        def _(r):
            gate = gate_buf[slot, span(r, 16), :].astype(F32)
            value = gate / (1.0 + jnp.exp(-gate)) * up_buf[slot, span(r, 16), :].astype(F32)
            hidden[pl.ds(pl.multiple_of(i * chunk + r * 16, 16), 16), :] = value.astype(BF16)

        if more:

            @pl.when(i + 2 < pieces)
            def _():
                gate_copy(i + 2).start()
                up_copy(i + 2).start()

    def partial(i, fresh):
        @pl.loop(1, tp)
        def _(k):
            @pl.loop(0, tiles)
            def _(n):
                if fresh:
                    weight_copy(k, n).wait()
                product = jnp.dot(
                    hidden[token_rows(i), :], held[k, :, span(n, tile)], preferred_element_type=F32
                ) * scale
                top = product.astype(BF16)
                high_out[k - 1, token_rows(i), span(n, tile)] = top
                low_out[k - 1, token_rows(i), span(n, tile)] = (product - top.astype(F32)).astype(BF16)

    def send_high(i):
        for k in range(1, tp):
            high_copy(k, i).start()

    begin(0, False)
    for i in range(1, min(3, pieces)):
        gate_copy(i).start()
        up_copy(i).start()
    weight_start(0)
    goal_copy.start()
    partial(0, True)
    pl.semaphore_wait(barrier, tp + 2)

    @pl.when(odd == 1)
    def _():
        send_high(0)

    @pl.loop(1, pieces)
    def _(i):
        begin(i, True)
        partial(i, False)

        @pl.when(odd == 1)
        def _():
            send_high(i)

    def sent_high(i):
        for k in range(1, tp):
            high_copy(k, i).wait_send()

    def hand_over():
        pl.semaphore_signal(turn_sem, inc=1, device_id=partner, device_id_type=MESH)

    @pl.when(odd == 1)
    def _():
        pl.loop(0, max(pieces - 2, 0))(sent_high)
        hand_over()

    @pl.when(odd == 0)
    def _():
        pl.semaphore_wait(turn_sem, 1)
        pl.loop(0, window)(send_high)

    goal_copy.wait()

    @pl.loop(0, tokens // group)
    def _(i):
        @pl.loop(0, tiles)
        def _(n):
            @pl.when(i == 0)
            def _():
                weight_copy(0, n).wait()

            share[span(i, group), span(n, tile)] = jnp.dot(
                hidden[span(i, group), :], held[0, :, span(n, tile)], preferred_element_type=F32
            ) * scale

    flat[...] = jnp.zeros_like(flat)
    lane = lax.broadcasted_iota(jnp.int32, (step, 128), 1)

    def stat_copy(turn, k, i):
        return pltpu.make_async_remote_copy(
            src_ref=stat_out.at[turn, i],
            dst_ref=stat_in.at[turn, k - 1, i],
            send_sem=stat_send.at[turn, k - 1, i],
            recv_sem=stat_recv.at[turn, k - 1, i],
            device_id=peer(k),
            device_id_type=MESH,
        )

    def add_and_count(turn, landing, i):
        @pl.loop(0, chunk // step)
        def _(r):
            here = pl.ds(pl.multiple_of(i * chunk + r * step, step), step)
            total = share[here, :]
            for k in range(1, tp):
                total = total + landing[k - 1, here, :].astype(F32)
            share[here, :] = total
            gain = gain_ref[...]
            squares = total * total
            first = jnp.sum(squares, axis=1, keepdims=True)
            second = jnp.sum(squares * (gain * gain), axis=1, keepdims=True)
            third = jnp.sum(total * (goal[here, :].astype(F32) * gain), axis=1, keepdims=True)
            turned[span(r, step), :] = jnp.where(
                lane == 0, first, jnp.where(lane == 1, second, jnp.where(lane == 2, third, 0.0))
            )

        stat_out[turn, i] = turned[...].T[0:8, :]
        for k in range(1, tp):
            stat_copy(turn, k, i).start()

    def gradient(turn, result, i):
        totals = stat_out[turn, i]
        for k in range(1, tp):
            stat_copy(turn, k, i).wait()
            totals = totals + stat_in[turn, k - 1, i]
        flat[0:8, :] = totals
        turned[...] = flat[...].T

        @pl.loop(0, chunk // step)
        def _(r):
            here = pl.ds(pl.multiple_of(i * chunk + r * step, step), step)
            sums = turned[span(r, step), :] * (1.0 / width)
            inv_rms = lax.rsqrt(sums[:, 0:1] + EPSILON)
            inner = inv_rms * (inv_rms * sums[:, 1:2] - sums[:, 2:3])
            gain = gain_ref[...]
            normal = share[here, :] * inv_rms
            output = normal * gain
            grad_norm = (output - goal[here, :].astype(F32)) * gain
            result[here, :] = (inv_rms * (grad_norm - normal * inner)).astype(BF16)
            if turn:
                normed[here, :] = output.astype(BF16)

    def block_copy(k, b):
        return pltpu.make_async_remote_copy(
            src_ref=held.at[k, span(b, block)],
            dst_ref=inbox.at[k, span(b, block)],
            send_sem=block_send.at[k, b],
            recv_sem=block_recv.at[k, b],
            device_id=ahead,
            device_id_type=MESH,
        )

    def update(k, b, grad):
        @pl.loop(0, tiles)
        def _(n):
            weight_grad = lax.dot_general(
                hidden[:, span(b, block)], grad[:, span(n, tile)], (((0,), (0,)), ((), ())),
                preferred_element_type=F32,
            ) * scale
            old = held[k, span(b, block), span(n, tile)].astype(F32)
            held[k, span(b, block), span(n, tile)] = (old - rate * weight_grad).astype(BF16)

        block_copy(k, b).start()

    def count_high(i):
        for k in range(1, tp):
            high_copy(k, i).wait_recv()
        add_and_count(0, high_in, i)

    def coarse_gradient(i):
        gradient(0, coarse, i)

    pl.loop(0, window - 1)(count_high)

    @pl.when(odd == 0)
    def _():
        pl.loop(window, pieces)(send_high)

    pl.loop(window - 1, min(window, pieces - 1))(count_high)
    pl.loop(0, window - 1)(coarse_gradient)
    pl.loop(min(window, pieces - 1), pieces)(count_high)

    def send_low():
        for k in range(1, tp):
            for i in range(pieces):
                low_copy(k, i).start()

    @pl.when(odd == 0)
    def _():
        pl.loop(0, pieces)(sent_high)
        hand_over()
        send_low()

    @pl.when(odd == 1)
    def _():
        pl.loop(max(pieces - 2, 0), pieces)(sent_high)

    pl.loop(window - 1, pieces)(coarse_gradient)

    @pl.loop(0, early)
    def _(b):
        update(0, b, coarse)

    @pl.when(odd == 1)
    def _():
        pl.semaphore_wait(turn_sem, 1)
        send_low()

    @pl.loop(0, pieces)
    def _(i):
        for k in range(1, tp):
            low_copy(k, i).wait()
        add_and_count(1, low_in, i)

    def grad_copy(k):
        return pltpu.make_async_remote_copy(
            src_ref=grads.at[0],
            dst_ref=grads.at[tp - k],
            send_sem=grad_send.at[k - 1],
            recv_sem=grad_recv.at[tp - k - 1],
            device_id=peer(k),
            device_id_type=MESH,
        )

    @pl.loop(0, pieces)
    def _(i):
        gradient(1, grads.at[0], i)

    for k in range(1, tp):
        grad_copy(k).start()

    @pl.loop(early, blocks)
    def _(b):
        update(0, b, grads.at[0])

    for k in range(1, tp):
        grad_copy(k).wait()

    @pl.loop(1, tp)
    def _(k):
        @pl.loop(0, blocks)
        def _(b):
            update(k, b, grads.at[k])

    @pl.loop(0, tp)
    def _(k):
        @pl.loop(0, blocks)
        def _(b):
            block_copy(k, b).wait()

            @pl.loop(0, block // 16)
            def _(r):
                here = pl.ds(pl.multiple_of(b * block + r * 16, 16), 16)
                both = held[k, here, :].astype(F32) + inbox[k, here, :].astype(F32)
                held[k, here, :] = (0.5 * both).astype(BF16)


def write_out(parts, normed_ref, held_ref, normed_hbm, mixed_hbm, normed_sem, mixed_sem):
    tp, rows, part = held_ref.shape
    me = lax.axis_index("tp")
    copies = [pltpu.make_async_copy(normed_ref, normed_hbm, normed_sem)]
    for k in range(tp):
        columns = pl.ds(pl.multiple_of(lax.rem(me + k, tp) * part, part), part)
        for i in range(parts):
            here = pl.ds(i * (rows // parts), rows // parts)
            copies.append(
                pltpu.make_async_copy(
                    held_ref.at[k, here], mixed_hbm.at[here, columns], mixed_sem.at[k, i]
                )
            )
    for copy in copies:
        copy.start()
    for copy in copies:
        copy.wait()


def shards(gate_pre, up_pre, target, norm_gain, weight, round_index):
    rate = step_rate(round_index)
    replicas = lax.axis_size("dp")
    levels = replicas.bit_length() - 1
    level = round_index[0] % levels
    tp = lax.axis_size("tp")
    _, rows, width = weight.shape
    tokens = gate_pre.shape[0]
    part = width // tp
    scale = (rows * tp) ** (-0.5)
    chunk, group = divisor(tokens, (128,)), divisor(tokens, (256, 128))
    tile = divisor(part, (256, 128))
    block = divisor(rows, (256, 128))
    pieces, blocks = tokens // chunk, rows // block
    dma = pltpu.SemaphoreType.DMA

    def call(bit):
        shares = ((0, 8), (3, 6), (3, 6), (2, 3))[min(bit, 3)]
        early = [blocks * share // 14 for share in shares]
        any_space = pl.BlockSpec(memory_space=pl.ANY)
        return pl.pallas_call(
            functools.partial(kernel, 1 << bit, *early, chunk, group, tile, block, scale),
            out_shape=(pltpu.VMEM((tokens, part), BF16), pltpu.VMEM((tp, rows, part), BF16)),
            in_specs=[
                pl.BlockSpec(memory_space=pltpu.SMEM),
                pl.BlockSpec(memory_space=pltpu.VMEM),
            ]
            + [any_space] * 4,
            out_specs=(pl.BlockSpec(memory_space=pltpu.VMEM),) * 2,
            scratch_shapes=[
                pltpu.VMEM((tp, rows, part), BF16),
                pltpu.VMEM((tokens, rows), BF16),
                pltpu.VMEM((2, chunk, rows), BF16),
                pltpu.VMEM((2, chunk, rows), BF16),
            ]
            + [pltpu.VMEM((tp - 1, tokens, part), BF16)] * 4
            + [
                pltpu.VMEM((tokens, part), F32),
                pltpu.VMEM((tokens, part), BF16),
                pltpu.VMEM((tp, tokens, part), BF16),
                pltpu.VMEM((tokens, part), BF16),
                pltpu.VMEM((chunk, 128), F32),
                pltpu.VMEM((128, chunk), F32),
                pltpu.VMEM((2, pieces, 8, chunk), F32),
                pltpu.VMEM((2, tp - 1, pieces, 8, chunk), F32),
                dma((2,)),
                dma((2,)),
                dma((tp, part // tile)),
                dma,
            ]
            + [dma((tp - 1, pieces))] * 4
            + [dma((2, tp - 1, pieces))] * 2
            + [dma((tp - 1,))] * 2
            + [dma((tp, blocks))] * 2
            + [pltpu.SemaphoreType.REGULAR],
            compiler_params=pltpu.CompilerParams(
                collective_id=bit, has_side_effects=True, vmem_limit_bytes=49_000_000
            ),
            name=f"step_level{bit}",
        )

    def write(normed, held):
        any_space = pl.BlockSpec(memory_space=pl.ANY)
        parts = 4
        return pl.pallas_call(
            functools.partial(write_out, parts),
            out_shape=(
                jax.ShapeDtypeStruct((tokens, part), BF16),
                jax.ShapeDtypeStruct((rows, width), BF16),
            ),
            in_specs=[pl.BlockSpec(memory_space=pltpu.VMEM)] * 2,
            out_specs=(any_space, any_space),
            scratch_shapes=[dma, dma((tp, parts))],
            compiler_params=pltpu.CompilerParams(
                has_side_effects=True, vmem_limit_bytes=2_000_000
            ),
            name="write_out",
        )(*(pltpu.with_memory_space_constraint(x, pltpu.VMEM) for x in (normed, held)))

    def branch(bit):
        def run(*operands):
            normed, held = call(bit)(*operands)
            return write(normed, held)

        return run

    normed, mixed = lax.switch(
        level,
        [branch(bit) for bit in range(levels)],
        rate[None],
        norm_gain[None, :],
        gate_pre,
        up_pre,
        target,
        weight[0],
    )
    return (normed, mixed[None])


def solution(mesh):
    return jax.shard_map(
        shards,
        mesh=mesh,
        in_specs=(P("dp", "tp"), P("dp", "tp"), P("dp", "tp"), P("tp"), P("dp", "tp", None), P()),
        out_specs=(P("dp", "tp"), P("dp", "tp", None)),
        check_vma=False,
    )
```

```python
import functools
import math

import jax
import jax.numpy as jnp
from jax import lax
from jax.experimental import pallas as pl
from jax.experimental.pallas import tpu as pltpu
from jax.sharding import PartitionSpec as P

EPSILON = 1e-06
MESH = pl.DeviceIdType.MESH
BF16, F32 = jnp.bfloat16, jnp.float32


def step_rate(round_index):
    phase = (round_index[0] % 1000).astype(jnp.float32) * jnp.float32(2.0 * math.pi / 1000.0)
    return jnp.float32(0.25) * (jnp.float32(0.55) + jnp.float32(0.45) * jnp.cos(phase))


def divisor(size, limits):
    for limit in limits:
        if size % limit == 0:
            return limit
    return size


def kernel(
    offset, early_even, early_odd, chunk, group, tile, block, scale,
    rate_ref, gain_ref, gate_hbm, up_hbm, target_hbm, weight_hbm,
    normed, held,
    inbox, hidden, gate_buf, up_buf, high_out, low_out, high_in, low_in,
    share, goal, grads, coarse, turned, flat, stat_out, stat_in,
    gate_sem, up_sem, weight_sem, goal_sem, high_send, high_recv, low_send, low_recv,
    stat_send, stat_recv, grad_send, grad_recv, block_send, block_recv, turn_sem,
):
    tp, rows, part = held.shape
    tokens = hidden.shape[0]
    width = tp * part
    pieces, tiles, blocks = tokens // chunk, part // tile, rows // block
    window, step = max(pieces - 1, 1), 64
    me, mine = lax.axis_index("tp"), lax.axis_index("dp")
    replicas = lax.axis_size("dp")
    ahead = {"dp": lax.rem(mine + offset, replicas)}
    behind = {"dp": lax.rem(mine + replicas - offset, replicas)}
    odd = lax.rem(mine, 2)
    partner = {"dp": mine + 1 - 2 * odd}
    early = early_odd * odd + early_even * (1 - odd)
    rate = rate_ref[0]

    def peer(k):
        return {"tp": lax.rem(me + k, tp)}

    def columns(k):
        return pl.ds(pl.multiple_of(lax.rem(me + k, tp) * part, part), part)

    def token_rows(i):
        return pl.ds(pl.multiple_of(i * chunk, chunk), chunk)

    def span(i, size):
        return pl.ds(pl.multiple_of(i * size, size), size)

    barrier = pltpu.get_barrier_semaphore()
    for k in range(1, tp):
        pl.semaphore_signal(barrier, inc=1, device_id=peer(k), device_id_type=MESH)
    pl.semaphore_signal(barrier, inc=1, device_id=ahead, device_id_type=MESH)
    pl.semaphore_signal(barrier, inc=1, device_id=behind, device_id_type=MESH)
    pl.semaphore_signal(barrier, inc=1, device_id=partner, device_id_type=MESH)

    def gate_copy(i):
        slot = lax.rem(i, 2)
        return pltpu.make_async_copy(gate_hbm.at[token_rows(i)], gate_buf.at[slot], gate_sem.at[slot])

    def up_copy(i):
        slot = lax.rem(i, 2)
        return pltpu.make_async_copy(up_hbm.at[token_rows(i)], up_buf.at[slot], up_sem.at[slot])

    def weight_copy(k, n):
        first = lax.rem(me + k, tp) * part + n * tile
        return pltpu.make_async_copy(
            weight_hbm.at[:, pl.ds(pl.multiple_of(first, tile), tile)],
            held.at[k, :, span(n, tile)],
            weight_sem.at[k, n],
        )

    def weight_start(k):
        for n in range(tiles):
            weight_copy(k, n).start()

    goal_copy = pltpu.make_async_copy(target_hbm, goal, goal_sem)
    gate_copy(0).start()
    up_copy(0).start()
    for k in range(1, tp):
        weight_start(k)

    def tp_copy(source, landing, send, recv, k, i):
        return pltpu.make_async_remote_copy(
            src_ref=source.at[k - 1, token_rows(i)],
            dst_ref=landing.at[k - 1, token_rows(i)],
            send_sem=send.at[k - 1, i],
            recv_sem=recv.at[k - 1, i],
            device_id=peer(k),
            device_id_type=MESH,
        )

    def high_copy(k, i):
        return tp_copy(high_out, high_in, high_send, high_recv, k, i)

    def low_copy(k, i):
        return tp_copy(low_out, low_in, low_send, low_recv, k, i)

    def begin(i, more):
        slot = lax.rem(i, 2)
        gate_copy(i).wait()
        up_copy(i).wait()

        @pl.loop(0, chunk // 16)
        def _(r):
            gate = gate_buf[slot, span(r, 16), :].astype(F32)
            value = gate / (1.0 + jnp.exp(-gate)) * up_buf[slot, span(r, 16), :].astype(F32)
            hidden[pl.ds(pl.multiple_of(i * chunk + r * 16, 16), 16), :] = value.astype(BF16)

        if more:

            @pl.when(i + 2 < pieces)
            def _():
                gate_copy(i + 2).start()
                up_copy(i + 2).start()

    def partial(i, fresh):
        @pl.loop(1, tp)
        def _(k):
            @pl.loop(0, tiles)
            def _(n):
                if fresh:
                    weight_copy(k, n).wait()
                product = jnp.dot(
                    hidden[token_rows(i), :], held[k, :, span(n, tile)], preferred_element_type=F32
                ) * scale
                top = product.astype(BF16)
                high_out[k - 1, token_rows(i), span(n, tile)] = top
                low_out[k - 1, token_rows(i), span(n, tile)] = (product - top.astype(F32)).astype(BF16)

    def send_high(i):
        for k in range(1, tp):
            high_copy(k, i).start()

    begin(0, False)
    for i in range(1, min(3, pieces)):
        gate_copy(i).start()
        up_copy(i).start()
    weight_start(0)
    goal_copy.start()
    partial(0, True)
    pl.semaphore_wait(barrier, tp + 2)

    @pl.when(odd == 1)
    def _():
        send_high(0)

    @pl.loop(1, pieces)
    def _(i):
        begin(i, True)
        partial(i, False)

        @pl.when(odd == 1)
        def _():
            send_high(i)

    def sent_high(i):
        for k in range(1, tp):
            high_copy(k, i).wait_send()

    def hand_over():
        pl.semaphore_signal(turn_sem, inc=1, device_id=partner, device_id_type=MESH)

    @pl.when(odd == 1)
    def _():
        pl.loop(0, max(pieces - 2, 0))(sent_high)
        hand_over()

    @pl.when(odd == 0)
    def _():
        pl.semaphore_wait(turn_sem, 1)
        pl.loop(0, window)(send_high)

    goal_copy.wait()
    flat[...] = jnp.zeros_like(flat)
    lane = lax.broadcasted_iota(jnp.int32, (step, 128), 1)

    def stat_copy(turn, k, i):
        return pltpu.make_async_remote_copy(
            src_ref=stat_out.at[turn, i],
            dst_ref=stat_in.at[turn, k - 1, i],
            send_sem=stat_send.at[turn, k - 1, i],
            recv_sem=stat_recv.at[turn, k - 1, i],
            device_id=peer(k),
            device_id_type=MESH,
        )

    def add_and_count(turn, landing, i):
        @pl.loop(0, chunk // step)
        def _(r):
            here = pl.ds(pl.multiple_of(i * chunk + r * step, step), step)
            total = share[here, :]
            for k in range(1, tp):
                total = total + landing[k - 1, here, :].astype(F32)
            share[here, :] = total
            gain = gain_ref[...]
            squares = total * total
            first = jnp.sum(squares, axis=1, keepdims=True)
            second = jnp.sum(squares * (gain * gain), axis=1, keepdims=True)
            third = jnp.sum(total * (goal[here, :].astype(F32) * gain), axis=1, keepdims=True)
            turned[span(r, step), :] = jnp.where(
                lane == 0, first, jnp.where(lane == 1, second, jnp.where(lane == 2, third, 0.0))
            )

        stat_out[turn, i] = turned[...].T[0:8, :]
        for k in range(1, tp):
            stat_copy(turn, k, i).start()

    def gradient(turn, result, i):
        totals = stat_out[turn, i]
        for k in range(1, tp):
            stat_copy(turn, k, i).wait()
            totals = totals + stat_in[turn, k - 1, i]
        flat[0:8, :] = totals
        turned[...] = flat[...].T

        @pl.loop(0, chunk // step)
        def _(r):
            here = pl.ds(pl.multiple_of(i * chunk + r * step, step), step)
            sums = turned[span(r, step), :] * (1.0 / width)
            inv_rms = lax.rsqrt(sums[:, 0:1] + EPSILON)
            inner = inv_rms * (inv_rms * sums[:, 1:2] - sums[:, 2:3])
            gain = gain_ref[...]
            normal = share[here, :] * inv_rms
            output = normal * gain
            grad_norm = (output - goal[here, :].astype(F32)) * gain
            result[here, :] = (inv_rms * (grad_norm - normal * inner)).astype(BF16)
            if turn:
                normed[here, :] = output.astype(BF16)

    def block_copy(k, b):
        return pltpu.make_async_remote_copy(
            src_ref=held.at[k, span(b, block)],
            dst_ref=inbox.at[k, span(b, block)],
            send_sem=block_send.at[k, b],
            recv_sem=block_recv.at[k, b],
            device_id=ahead,
            device_id_type=MESH,
        )

    def update(k, b, grad):
        @pl.loop(0, tiles)
        def _(n):
            weight_grad = lax.dot_general(
                hidden[:, span(b, block)], grad[:, span(n, tile)], (((0,), (0,)), ((), ())),
                preferred_element_type=F32,
            ) * scale
            old = held[k, span(b, block), span(n, tile)].astype(F32)
            held[k, span(b, block), span(n, tile)] = (old - rate * weight_grad).astype(BF16)

        block_copy(k, b).start()

    def count_high(i):
        for k in range(1, tp):
            high_copy(k, i).wait_recv()
        add_and_count(0, high_in, i)

    def coarse_gradient(i):
        gradient(0, coarse, i)

    @pl.loop(0, tokens // group)
    def _(g):
        @pl.loop(0, tiles)
        def _(n):
            @pl.when(g == 0)
            def _():
                weight_copy(0, n).wait()

            share[span(g, group), span(n, tile)] = jnp.dot(
                hidden[span(g, group), :], held[0, :, span(n, tile)], preferred_element_type=F32
            ) * scale

        pl.loop(g * (group // chunk), (g + 1) * (group // chunk))(count_high)

        @pl.when((g == 0) & (odd == 0))
        def _():
            pl.loop(window, pieces)(send_high)

    def send_low():
        for k in range(1, tp):
            for i in range(pieces):
                low_copy(k, i).start()

    @pl.when(odd == 0)
    def _():
        pl.loop(0, pieces)(sent_high)
        hand_over()

    @pl.when(odd == 1)
    def _():
        pl.loop(max(pieces - 2, 0), pieces)(sent_high)

    pl.loop(0, pieces)(coarse_gradient)

    @pl.loop(0, early)
    def _(b):
        update(0, b, coarse)

    pl.semaphore_wait(turn_sem, 1)
    send_low()

    @pl.loop(0, pieces)
    def _(i):
        for k in range(1, tp):
            low_copy(k, i).wait()

        @pl.when((odd == 1) & (i == max(pieces - 2, 0)))
        def _():
            hand_over()

        add_and_count(1, low_in, i)

    def grad_copy(k):
        return pltpu.make_async_remote_copy(
            src_ref=grads.at[0],
            dst_ref=grads.at[tp - k],
            send_sem=grad_send.at[k - 1],
            recv_sem=grad_recv.at[tp - k - 1],
            device_id=peer(k),
            device_id_type=MESH,
        )

    @pl.loop(0, pieces)
    def _(i):
        gradient(1, grads.at[0], i)

    for k in range(1, tp):
        grad_copy(k).start()

    @pl.loop(early, blocks)
    def _(b):
        update(0, b, grads.at[0])

    for k in range(1, tp):
        grad_copy(k).wait()

    @pl.loop(1, tp)
    def _(k):
        @pl.loop(0, blocks)
        def _(b):
            update(k, b, grads.at[k])

    @pl.loop(0, tp)
    def _(k):
        @pl.loop(0, blocks)
        def _(b):
            block_copy(k, b).wait()

            @pl.loop(0, block // 16)
            def _(r):
                here = pl.ds(pl.multiple_of(b * block + r * 16, 16), 16)
                both = held[k, here, :].astype(F32) + inbox[k, here, :].astype(F32)
                held[k, here, :] = (0.5 * both).astype(BF16)


def write_out(parts, normed_ref, held_ref, normed_hbm, mixed_hbm, normed_sem, mixed_sem):
    tp, rows, part = held_ref.shape
    me = lax.axis_index("tp")
    copies = [pltpu.make_async_copy(normed_ref, normed_hbm, normed_sem)]
    for k in range(tp):
        columns = pl.ds(pl.multiple_of(lax.rem(me + k, tp) * part, part), part)
        for i in range(parts):
            here = pl.ds(i * (rows // parts), rows // parts)
            copies.append(
                pltpu.make_async_copy(
                    held_ref.at[k, here], mixed_hbm.at[here, columns], mixed_sem.at[k, i]
                )
            )
    for copy in copies:
        copy.start()
    for copy in copies:
        copy.wait()


def shards(gate_pre, up_pre, target, norm_gain, weight, round_index):
    rate = step_rate(round_index)
    replicas = lax.axis_size("dp")
    levels = replicas.bit_length() - 1
    level = round_index[0] % levels
    tp = lax.axis_size("tp")
    _, rows, width = weight.shape
    tokens = gate_pre.shape[0]
    part = width // tp
    scale = (rows * tp) ** (-0.5)
    chunk, group = divisor(tokens, (128,)), divisor(tokens, (256, 128))
    tile = divisor(part, (256, 128))
    block = divisor(rows, (256, 128))
    pieces, blocks = tokens // chunk, rows // block
    dma = pltpu.SemaphoreType.DMA

    def call(bit):
        shares = ((0, 6), (3, 4), (3, 4), (2, 2))[min(bit, 3)]
        early = [blocks * share // 14 for share in shares]
        any_space = pl.BlockSpec(memory_space=pl.ANY)
        return pl.pallas_call(
            functools.partial(kernel, 1 << bit, *early, chunk, group, tile, block, scale),
            out_shape=(pltpu.VMEM((tokens, part), BF16), pltpu.VMEM((tp, rows, part), BF16)),
            in_specs=[
                pl.BlockSpec(memory_space=pltpu.SMEM),
                pl.BlockSpec(memory_space=pltpu.VMEM),
            ]
            + [any_space] * 4,
            out_specs=(pl.BlockSpec(memory_space=pltpu.VMEM),) * 2,
            scratch_shapes=[
                pltpu.VMEM((tp, rows, part), BF16),
                pltpu.VMEM((tokens, rows), BF16),
                pltpu.VMEM((2, chunk, rows), BF16),
                pltpu.VMEM((2, chunk, rows), BF16),
            ]
            + [pltpu.VMEM((tp - 1, tokens, part), BF16)] * 4
            + [
                pltpu.VMEM((tokens, part), F32),
                pltpu.VMEM((tokens, part), BF16),
                pltpu.VMEM((tp, tokens, part), BF16),
                pltpu.VMEM((tokens, part), BF16),
                pltpu.VMEM((chunk, 128), F32),
                pltpu.VMEM((128, chunk), F32),
                pltpu.VMEM((2, pieces, 8, chunk), F32),
                pltpu.VMEM((2, tp - 1, pieces, 8, chunk), F32),
                dma((2,)),
                dma((2,)),
                dma((tp, part // tile)),
                dma,
            ]
            + [dma((tp - 1, pieces))] * 4
            + [dma((2, tp - 1, pieces))] * 2
            + [dma((tp - 1,))] * 2
            + [dma((tp, blocks))] * 2
            + [pltpu.SemaphoreType.REGULAR],
            compiler_params=pltpu.CompilerParams(
                collective_id=bit, has_side_effects=True, vmem_limit_bytes=49_000_000
            ),
            name=f"step_level{bit}",
        )

    def write(normed, held):
        any_space = pl.BlockSpec(memory_space=pl.ANY)
        parts = 4
        return pl.pallas_call(
            functools.partial(write_out, parts),
            out_shape=(
                jax.ShapeDtypeStruct((tokens, part), BF16),
                jax.ShapeDtypeStruct((rows, width), BF16),
            ),
            in_specs=[pl.BlockSpec(memory_space=pltpu.VMEM)] * 2,
            out_specs=(any_space, any_space),
            scratch_shapes=[dma, dma((tp, parts))],
            compiler_params=pltpu.CompilerParams(
                has_side_effects=True, vmem_limit_bytes=2_000_000
            ),
            name="write_out",
        )(*(pltpu.with_memory_space_constraint(x, pltpu.VMEM) for x in (normed, held)))

    def branch(bit):
        def run(*operands):
            normed, held = call(bit)(*operands)
            return write(normed, held)

        return run

    normed, mixed = lax.switch(
        level,
        [branch(bit) for bit in range(levels)],
        rate[None],
        norm_gain[None, :],
        gate_pre,
        up_pre,
        target,
        weight[0],
    )
    return (normed, mixed[None])


def solution(mesh):
    return jax.shard_map(
        shards,
        mesh=mesh,
        in_specs=(P("dp", "tp"), P("dp", "tp"), P("dp", "tp"), P("tp"), P("dp", "tp", None), P()),
        out_specs=(P("dp", "tp"), P("dp", "tp", None)),
        check_vma=False,
    )
```
